32 devices in a mesh: tower: 2 (over x), blk: 16 (over z, y, core).
Axes of the slice: x: 2, y: 2, z: 4, core: 2. Of those that a mesh axis runs over, the one named last changes fastest.
Arguments:
- pooled: bfloat16 [2, 2048, 1152], P('tower', 'blk'), may hold values from -6 to 6
- final_gain: float32 [2, 1152], P('tower'), may hold values from 0.5 to 1.5
- head_weight: bfloat16 [2, 1152, 1152], P('tower'), may hold values from -0.1875 to 0.1875
- pair_ids: int32 [2048], replicated, may hold values from 0 to 2047
- log_scale: float32 [1], replicated, may hold values from 4.2 to 4.7
- bias: float32 [1], replicated, may hold values from -4 to -1
Outputs:
- emb_grad: float32 [2, 2048, 1152], P('tower', 'blk')
The draws below stay inside these ranges and needn't reach their ends.
Inputs may be any that keep to these rules, and one draw needn't show every extreme that they name: `pair_ids`: examples with equal ids form positive pairs; every example is a positive pair with its own image and text.
All inputs are finite; a program needn't handle non-finite values.
Results may differ from the reference program's by a relative error of at most 0.0043.
Values may be sent and summed in bfloat16 or wider, within the bound.
A program may use at most 192 MiB of HBM per device.

```python
import jax
import jax.numpy as jnp
from jax import lax

D = 1152
EX_DEV = 128
BATCH = 2048


def set_ends(entries, rng, low, top_value):
    extent = entries.shape
    place = [jax.random.randint(jax.random.fold_in(rng, axis), (), 0, extent[axis]) for axis in range(len(extent))]
    entries = entries.at[tuple(place)].set(low)
    longest = extent.index(max(extent))
    place[longest] = (place[longest] + 1) % extent[longest]
    return entries.at[tuple(place)].set(top_value)


def levels(rng, dims, split, low, high):
    def one(dim, blocks):
        steps = jax.random.uniform(jax.random.fold_in(jax.random.fold_in(rng, 6), dim), (blocks,), jnp.float32, low / len(split), high / len(split))
        return jnp.repeat(jnp.exp(steps), dims[dim] // blocks).reshape((-1,) + (1,) * (len(dims) - dim - 1))

    level = one(*split[0])
    for cut in split[1:]:
        level = level * one(*cut)
    return level


def bell_draw(rng, dims, width, bound, pieces=(), kind=jnp.bfloat16):
    array = width * jax.random.normal(rng, dims, jnp.float32)
    if pieces:
        array = array * levels(rng, dims, pieces, -0.22, 0.18)
    return jnp.clip(array, -bound, bound).astype(kind)


def setup_inputs(seed: int = 0) -> dict:
    key_list = jax.random.split(jax.random.key(seed), 7)
    pooled = bell_draw(key_list[0], (2, BATCH, D), 1.0, 6.0, ((0, 2), (1, 16)))
    final_gain = jnp.clip(0.5 + 1.0 * jax.random.uniform(key_list[1], (2, D), jnp.float32) ** levels(key_list[1], (2, D), ((0, 2),), -0.2, 0.2), 0.5, 1.5)
    head_weight = bell_draw(key_list[2], (2, D, D), D ** -0.5, 0.1875, ((0, 2),))
    pair_ids = set_ends(jax.random.randint(key_list[3], (BATCH,), 0, BATCH), jax.random.fold_in(key_list[3], 1), 0, BATCH - 1).astype(jnp.int32)
    log_scale = jnp.clip(jax.random.uniform(key_list[4], (1,), jnp.float32, 4.2, 4.7), 4.2, 4.7)
    bias = jnp.clip(jax.random.uniform(key_list[5], (1,), jnp.float32, -4.0, -1.0), -4.0, -1.0)
    return {"pooled": pooled, "final_gain": final_gain, "head_weight": head_weight, "pair_ids": pair_ids, "log_scale": log_scale, "bias": bias}


def embed_rows(feats, gain, weight):
    values = feats.astype(jnp.float32)
    center = values - lax.optimization_barrier(jnp.mean(values, axis=-1, keepdims=True))
    spread = lax.optimization_barrier(jnp.mean(center * center, axis=-1, keepdims=True))
    normed = (center * lax.rsqrt(spread + 1e-06) * gain).astype(jnp.bfloat16)
    head = jnp.dot(normed, weight, preferred_element_type=jnp.float32)
    length = lax.optimization_barrier(jnp.sum(head * head, axis=-1, keepdims=True))
    return (head * lax.rsqrt(length + 1e-06)).astype(jnp.bfloat16)

def pair_forces(fixed_rows, moving_rows, fixed_ids, moving_ids, scale, shift):
    logits = scale * lax.dot_general(fixed_rows, moving_rows, (((1,), (1,)), ((), ())), preferred_element_type=jnp.float32) + shift
    sign = jnp.where(fixed_ids[:, None] == moving_ids[None, :], jnp.float32(1.0), jnp.float32(-1.0))
    coef = (-sign * jax.nn.sigmoid(-sign * logits)).astype(jnp.bfloat16)
    return jnp.dot(coef, moving_rows, preferred_element_type=jnp.float32)

def reference(pooled, final_gain, head_weight, pair_ids, log_scale, bias):
    images = embed_rows(pooled[0], final_gain[0], head_weight[0])
    texts = embed_rows(pooled[1], final_gain[1], head_weight[1])
    scale = jnp.exp(log_scale[0])
    shift = bias[0]
    blocks = BATCH // EX_DEV
    id_blocks = pair_ids.reshape(blocks, EX_DEV)

    def image_block(item):
        rows, ids = item
        return pair_forces(rows, texts, ids, pair_ids, scale, shift)

    def text_block(item):
        rows, ids = item
        return pair_forces(rows, images, ids, pair_ids, scale, shift)
    image_grad = lax.map(image_block, (images.reshape(blocks, EX_DEV, D), id_blocks)).reshape(BATCH, D)
    text_grad = lax.map(text_block, (texts.reshape(blocks, EX_DEV, D), id_blocks)).reshape(BATCH, D)
    return jnp.stack([image_grad, text_grad])
```

```python
import functools

import jax
import jax.numpy as jnp
from jax import lax
from jax.experimental import pallas as pl
from jax.experimental.pallas import tpu as pltpu
from jax.sharding import PartitionSpec as P

MESH = pl.DeviceIdType.MESH


def grid_of(blocks):
    chips = blocks // 2
    across = 1
    while (2 * across) ** 2 <= chips and chips % (2 * across) == 0:
        across *= 2
    return chips // across, across


def by_distance(size):
    return [sorted(range(size), key=lambda other: (abs(other - here), other)) for here in range(size)]


def pick(table, here, step):
    value = jnp.int32(table[0][step])
    for place in range(1, len(table)):
        value = jnp.where(here == place, jnp.int32(table[place][step]), value)
    return value


def kernel(
    sizes, pooled, gain, ids, log_scale, bias, weight, out,
    held, local, weights, coef, weight_sem,
    got, sent_x, sent_up, sent_down, sent_right, sent_left, sent_core,
):
    depth, across, pieces = sizes
    rows = pooled.shape[0]
    part = rows // pieces
    tower = lax.axis_index("tower")
    mine = lax.axis_index("blk")
    core = lax.rem(mine, 2)
    chip = lax.div(mine, 2)
    y = lax.rem(chip, across)
    z = lax.div(chip, across)

    fetch = pltpu.make_async_copy(weight, weights, weight_sem)
    fetch.start()

    def at(z_to, y_to, core_to):
        return (z_to * across + y_to) * 2 + core_to

    up, down = at(z + 1, y, core), at(z - 1, y, core)
    right, left = at(z, y + 1, core), at(z, y - 1, core)
    twin = at(z, y, 1 - core)
    has_up, has_down = z < depth - 1, z > 0
    has_right, has_left = y < across - 1, y > 0

    barrier = pltpu.get_barrier_semaphore()

    def greet(tower_to, blk_to):
        pl.semaphore_signal(barrier, inc=1, device_id={"tower": tower_to, "blk": blk_to}, device_id_type=MESH)

    greet(1 - tower, mine)
    greet(tower, twin)
    for there, who in ((has_up, up), (has_down, down), (has_right, right), (has_left, left)):
        pl.when(there)(functools.partial(greet, tower, who))

    values = pooled[...].astype(jnp.float32)
    center = values - jnp.mean(values, axis=-1, keepdims=True)
    spread = jnp.mean(center * center, axis=-1, keepdims=True)
    normed = (center * lax.rsqrt(spread + 1e-06) * gain[...]).astype(jnp.bfloat16)
    fetch.wait()
    head = jnp.dot(normed, weights[...], preferred_element_type=jnp.float32)
    length = jnp.sum(head * head, axis=-1, keepdims=True)
    local[...] = (head * lax.rsqrt(length + 1e-06)).astype(jnp.bfloat16)

    count = (
        2
        + has_up.astype(jnp.int32)
        + has_down.astype(jnp.int32)
        + has_right.astype(jnp.int32)
        + has_left.astype(jnp.int32)
    )
    pl.semaphore_wait(barrier, count)

    def span(k):
        return pl.ds(k * part, part)

    def cross(k):
        return pltpu.make_async_remote_copy(
            src_ref=local.at[span(k)],
            dst_ref=held.at[mine, span(k)],
            send_sem=sent_x.at[k],
            recv_sem=got.at[mine, k],
            device_id={"tower": 1 - tower, "blk": mine},
            device_id_type=MESH,
        )

    def relay(block, k, sem, who):
        return pltpu.make_async_remote_copy(
            src_ref=held.at[block, span(k)],
            dst_ref=held.at[block, span(k)],
            send_sem=sem,
            recv_sem=got.at[block, k],
            device_id={"tower": tower, "blk": who},
            device_id_type=MESH,
        )

    for k in range(pieces):
        cross(k).start()

    z_table, y_table = by_distance(depth), by_distance(across)
    z_at = [pick(z_table, z, j) for j in range(depth)]
    y_at = [pick(y_table, y, i) for i in range(across)]

    def sends(j, i, k):
        z_from, y_from = z_at[j], y_at[i]
        block = at(z_from, y_from, core)
        found = [(None, relay(block, k, sent_core.at[j, i, k], twin))]
        if i == 0:
            found.append((has_up & (z_from <= z), relay(block, k, sent_up.at[j, k], up)))
            found.append((has_down & (z_from >= z), relay(block, k, sent_down.at[j, k], down)))
        found.append((has_right & (y_from <= y), relay(block, k, sent_right.at[j, i, k], right)))
        found.append((has_left & (y_from >= y), relay(block, k, sent_left.at[j, i, k], left)))
        return found[1:] + found[:1]

    def arrive(j, i, k):
        block = at(z_at[j], y_at[i], core)
        relay(block, k, sent_core.at[j, i, k], twin).wait_recv()
        for there, copy in sends(j, i, k):
            if there is None:
                copy.start()
            else:
                pl.when(there)(copy.start)

    scale = jnp.exp(jnp.full((1, rows), log_scale[0], jnp.float32))
    shift = bias[0]
    own_ids = jnp.transpose(jnp.broadcast_to(ids[pl.ds(mine, 1), :], (rows, rows)))
    out[...] = jnp.zeros_like(out)

    def forces(j, i):
        group = z_at[j] * across + y_at[i]
        other = 2 * group + 1 - core
        for k in range(pieces):
            relay(other, k, sent_core.at[j, i, k], twin).wait_recv()
        moving = held[pl.ds(2 * group, 2)].reshape(2 * rows, -1)
        dots = lax.dot_general(
            local[...], moving, (((1,), (1,)), ((), ())), preferred_element_type=jnp.float32
        )
        for half in range(2):
            logits = scale * dots[:, half * rows : (half + 1) * rows] + shift
            same = own_ids == ids[pl.ds(2 * group + half, 1), :]
            sign = jnp.where(same, jnp.float32(1.0), jnp.float32(-1.0))
            coef[:, half * rows : (half + 1) * rows] = (
                -sign / (1.0 + jnp.exp(sign * logits))
            ).astype(jnp.bfloat16)
        out[...] += jnp.dot(coef[...], moving, preferred_element_type=jnp.float32)

    waiting = []
    for wave in range(depth + across - 1):
        fresh = [(j, wave - j) for j in range(depth) if 0 <= wave - j < across]
        fresh.sort(key=lambda pair: pair[1])
        for k in range(pieces):
            for j, i in fresh:
                arrive(j, i, k)
            if waiting:
                forces(*waiting.pop(0))
        waiting += fresh
    for pair in waiting:
        forces(*pair)

    for k in range(pieces):
        cross(k).wait_send()
    for j in range(depth):
        for i in range(across):
            for k in range(pieces):
                for there, copy in sends(j, i, k):
                    if there is None:
                        copy.wait_send()
                    else:
                        pl.when(there)(copy.wait_send)


def solution(mesh):
    blocks = mesh.shape["blk"]
    depth, across = grid_of(blocks)
    pieces = 4 if blocks <= 16 else 1

    def on_device(pooled, final_gain, head_weight, pair_ids, log_scale, bias):
        _, rows, width = pooled.shape
        vmem = pl.BlockSpec(memory_space=pltpu.VMEM)
        smem = pl.BlockSpec(memory_space=pltpu.SMEM)
        dma = pltpu.SemaphoreType.DMA
        total = pl.pallas_call(
            functools.partial(kernel, (depth, across, pieces)),
            name="tower_forces",
            out_shape=jax.ShapeDtypeStruct((rows, width), jnp.float32),
            in_specs=[vmem, vmem, vmem, smem, smem, pl.BlockSpec(memory_space=pl.ANY)],
            out_specs=vmem,
            scratch_shapes=[
                pltpu.VMEM((blocks, rows, width), jnp.bfloat16),
                pltpu.VMEM((rows, width), jnp.bfloat16),
                pltpu.VMEM((width, width), jnp.bfloat16),
                pltpu.VMEM((rows, 2 * rows), jnp.bfloat16),
                dma,
                dma((blocks, pieces)),
                dma((pieces,)),
                dma((depth, pieces)),
                dma((depth, pieces)),
                dma((depth, across, pieces)),
                dma((depth, across, pieces)),
                dma((depth, across, pieces)),
            ],
            compiler_params=pltpu.CompilerParams(
                collective_id=0, has_side_effects=True, vmem_limit_bytes=60 * 2**20
            ),
        )(pooled[0], final_gain, pair_ids.reshape(blocks, rows), log_scale, bias, head_weight[0])
        return total[None]

    placed = (P("tower", "blk", None), P("tower", None), P("tower", None, None), P(), P(), P())
    return jax.shard_map(
        on_device, mesh=mesh, in_specs=placed, out_specs=P("tower", "blk", None), check_vma=False
    )
```

```python
import functools

import jax
import jax.numpy as jnp
from jax import lax
from jax.experimental import pallas as pl
from jax.experimental.pallas import tpu as pltpu
from jax.sharding import PartitionSpec as P

MESH = pl.DeviceIdType.MESH


def grid_of(blocks):
    chips = blocks // 2
    across = 1
    while (2 * across) ** 2 <= chips and chips % (2 * across) == 0:
        across *= 2
    return chips // across, across


def by_distance(size):
    return [sorted(range(size), key=lambda other: (abs(other - here), other)) for here in range(size)]


def pick(table, here, step):
    value = jnp.int32(table[0][step])
    for place in range(1, len(table)):
        value = jnp.where(here == place, jnp.int32(table[place][step]), value)
    return value


def kernel(
    sizes, log_scale, bias, pooled_hbm, gain_hbm, ids_hbm, weight, out,
    held, local, near, pooled, gain, ids, weights, head, coef, fetch_sem, weight_sem,
    got, near_got, sent_x, sent_near, sent_over, sent_level,
    sent_up, sent_down, sent_right, sent_left, sent_core,
):
    depth, across, pieces = sizes
    swap = across == 2
    level = swap and pieces > 1 and depth % 2 == 0
    rows, width = pooled.shape
    part = rows // pieces
    tower = lax.axis_index("tower")
    mine = lax.axis_index("blk")
    core = lax.rem(mine, 2)
    chip = lax.div(mine, 2)
    y = lax.rem(chip, across)
    z = lax.div(chip, across)

    fetches = [
        pltpu.make_async_copy(pooled_hbm, pooled, fetch_sem.at[0]),
        pltpu.make_async_copy(gain_hbm, gain, fetch_sem.at[1]),
        pltpu.make_async_copy(ids_hbm, ids, fetch_sem.at[2]),
    ]
    for fetch in fetches:
        fetch.start()
    slices = weight_sem.shape[0]
    columns = [pl.ds(s * (width // slices), width // slices) for s in range(slices)]
    weight_fetches = [
        pltpu.make_async_copy(weight.at[:, columns[s]], weights.at[:, columns[s]], weight_sem.at[s])
        for s in range(slices)
    ]
    for fetch in weight_fetches:
        fetch.start()

    def at(z_to, y_to, core_to):
        return (z_to * across + y_to) * 2 + core_to

    up, down = at(z + 1, y, core), at(z - 1, y, core)
    right, left = at(z, y + 1, core), at(z, y - 1, core)
    twin = at(z, y, 1 - core)
    has_up, has_down = z < depth - 1, z > 0
    has_right, has_left = y < across - 1, y > 0

    barrier = pltpu.get_barrier_semaphore()

    def greet(tower_to, blk_to):
        pl.semaphore_signal(barrier, inc=1, device_id={"tower": tower_to, "blk": blk_to}, device_id_type=MESH)

    greet(1 - tower, mine)
    greet(tower, twin)
    for there, who in ((has_up, up), (has_down, down), (has_right, right), (has_left, left)):
        pl.when(there)(functools.partial(greet, tower, who))

    fetches[0].wait()
    fetches[1].wait()
    values = pooled[...].astype(jnp.float32)
    center = values - jnp.mean(values, axis=-1, keepdims=True)
    spread = jnp.mean(center * center, axis=-1, keepdims=True)
    normed = (center * lax.rsqrt(spread + 1e-06) * gain[...]).astype(jnp.bfloat16)
    length = jnp.zeros((rows, 1), jnp.float32)
    for s in range(slices):
        weight_fetches[s].wait()
        piece = jnp.dot(normed, weights[:, columns[s]], preferred_element_type=jnp.float32)
        length += jnp.sum(piece * piece, axis=-1, keepdims=True)
        head[:, columns[s]] = piece
    local[...] = (head[...] * lax.rsqrt(length + 1e-06)).astype(jnp.bfloat16)

    count = (
        2
        + has_up.astype(jnp.int32)
        + has_down.astype(jnp.int32)
        + has_right.astype(jnp.int32)
        + has_left.astype(jnp.int32)
    )
    pl.semaphore_wait(barrier, count)

    def span(k):
        return pl.ds(k * part, part)

    def cross(k):
        return pltpu.make_async_remote_copy(
            src_ref=local.at[span(k)],
            dst_ref=held.at[mine, span(k)],
            send_sem=sent_x.at[k],
            recv_sem=got.at[mine, k],
            device_id={"tower": 1 - tower, "blk": mine},
            device_id_type=MESH,
        )

    def relay(block, k, sem, who):
        return pltpu.make_async_remote_copy(
            src_ref=held.at[block, span(k)],
            dst_ref=held.at[block, span(k)],
            send_sem=sem,
            recv_sem=got.at[block, k],
            device_id={"tower": tower, "blk": who},
            device_id_type=MESH,
        )

    beside = at(z, 1 - y, core)

    def step_near(k):
        return pltpu.make_async_remote_copy(
            src_ref=local.at[span(k)],
            dst_ref=near.at[span(k)],
            send_sem=sent_near.at[k],
            recv_sem=near_got.at[k],
            device_id={"tower": tower, "blk": beside},
            device_id_type=MESH,
        )

    def step_over(k):
        return pltpu.make_async_remote_copy(
            src_ref=near.at[span(k)],
            dst_ref=held.at[beside, span(k)],
            send_sem=sent_over.at[k],
            recv_sem=got.at[beside, k],
            device_id={"tower": 1 - tower, "blk": mine},
            device_id_type=MESH,
        )

    pair_z = z + 1 - 2 * lax.rem(z, 2)

    def step_level():
        return relay(beside, pieces - 1, sent_level.at[0], at(pair_z, y, core))

    for k in range(pieces):
        cross(k).start()
        if swap:
            step_near(k).start()

    z_table, y_table = by_distance(depth), by_distance(across)
    z_at = [pick(z_table, z, j) for j in range(depth)]
    y_at = [pick(y_table, y, i) for i in range(across)]

    def sends(j, i, k):
        z_from, y_from = z_at[j], y_at[i]
        block = at(z_from, y_from, core)
        found = [(None, relay(block, k, sent_core.at[j, i, k], twin))]
        if i == 0:
            found.append((has_up & (z_from <= z), relay(block, k, sent_up.at[j, k], up)))
            found.append((has_down & (z_from >= z), relay(block, k, sent_down.at[j, k], down)))
        if not (swap and j == 0):
            over = True
            if level and i == 0 and k == pieces - 1:
                over = z_from != pair_z
            found.append((has_right & (y_from <= y) & over, relay(block, k, sent_right.at[j, i, k], right)))
            found.append((has_left & (y_from >= y) & over, relay(block, k, sent_left.at[j, i, k], left)))
        if level and j == 0 and i == 1 and k == pieces - 1:
            found.append((None, step_level()))
        return found[1:] + found[:1]

    def arrive(j, i, k):
        block = at(z_at[j], y_at[i], core)
        relay(block, k, sent_core.at[j, i, k], twin).wait_recv()
        for there, copy in sends(j, i, k):
            if there is None:
                copy.start()
            else:
                pl.when(there)(copy.start)

    fetches[2].wait()
    scale = jnp.exp(jnp.full((1, rows), log_scale[0], jnp.float32))
    shift = bias[0]
    own_ids = jnp.transpose(jnp.broadcast_to(ids[pl.ds(mine, 1), :], (rows, rows)))
    out[...] = jnp.zeros_like(out)

    def forces(j, i):
        group = z_at[j] * across + y_at[i]
        other = 2 * group + 1 - core
        for k in range(pieces):
            relay(other, k, sent_core.at[j, i, k], twin).wait_recv()
        moving = held[pl.ds(2 * group, 2)].reshape(2 * rows, -1)
        dots = lax.dot_general(
            local[...], moving, (((1,), (1,)), ((), ())), preferred_element_type=jnp.float32
        )
        for half in range(2):
            logits = scale * dots[:, half * rows : (half + 1) * rows] + shift
            same = own_ids == ids[pl.ds(2 * group + half, 1), :]
            sign = jnp.where(same, jnp.float32(1.0), jnp.float32(-1.0))
            coef[:, half * rows : (half + 1) * rows] = (
                -sign / (1.0 + jnp.exp(sign * logits))
            ).astype(jnp.bfloat16)
        out[...] += jnp.dot(coef[...], moving, preferred_element_type=jnp.float32)

    waiting = []
    for wave in range(depth + across - 1):
        fresh = [(j, wave - j) for j in range(depth) if 0 <= wave - j < across]
        fresh.sort(key=lambda pair: pair[1])
        for k in range(pieces):
            if swap and wave == 0:
                step_near(k).wait_recv()
                step_over(k).start()
            for j, i in fresh:
                arrive(j, i, k)
            if waiting:
                forces(*waiting.pop(0))
        waiting += fresh
    for pair in waiting:
        forces(*pair)

    for k in range(pieces):
        cross(k).wait_send()
        if swap:
            step_near(k).wait_send()
            step_over(k).wait_send()
    for j in range(depth):
        for i in range(across):
            for k in range(pieces):
                for there, copy in sends(j, i, k):
                    if there is None:
                        copy.wait_send()
                    else:
                        pl.when(there)(copy.wait_send)


def solution(mesh):
    blocks = mesh.shape["blk"]
    depth, across = grid_of(blocks)
    pieces = 4 if blocks <= 16 else 1

    def on_device(pooled, final_gain, head_weight, pair_ids, log_scale, bias):
        _, rows, width = pooled.shape
        smem = pl.BlockSpec(memory_space=pltpu.SMEM)
        hbm = pl.BlockSpec(memory_space=pltpu.HBM)
        dma = pltpu.SemaphoreType.DMA
        slices = 3 if width % 384 == 0 else 1
        grant = 67043328 - 4 * rows * width - 2**17
        total = pl.pallas_call(
            functools.partial(kernel, (depth, across, pieces)),
            name="tower_forces",
            out_shape=pltpu.VMEM((rows, width), jnp.float32),
            in_specs=[smem, smem, hbm, hbm, hbm, hbm],
            out_specs=pl.BlockSpec(memory_space=pltpu.VMEM),
            scratch_shapes=[
                pltpu.VMEM((blocks, rows, width), jnp.bfloat16),
                pltpu.VMEM((rows, width), jnp.bfloat16),
                pltpu.VMEM((rows, width), jnp.bfloat16),
                pltpu.VMEM((rows, width), jnp.bfloat16),
                pltpu.VMEM((1, width), jnp.float32),
                pltpu.VMEM((blocks, rows), jnp.int32),
                pltpu.VMEM((width, width), jnp.bfloat16),
                pltpu.VMEM((rows, width), jnp.float32),
                pltpu.VMEM((rows, 2 * rows), jnp.bfloat16),
                dma((3,)),
                dma((slices,)),
                dma((blocks, pieces)),
                dma((pieces,)),
                dma((pieces,)),
                dma((pieces,)),
                dma((pieces,)),
                dma((1,)),
                dma((depth, pieces)),
                dma((depth, pieces)),
                dma((depth, across, pieces)),
                dma((depth, across, pieces)),
                dma((depth, across, pieces)),
            ],
            compiler_params=pltpu.CompilerParams(
                collective_id=0, has_side_effects=True, vmem_limit_bytes=grant
            ),
        )(log_scale, bias, pooled[0], final_gain, pair_ids.reshape(blocks, rows), head_weight[0])
        return total[None]

    placed = (P("tower", "blk", None), P("tower", None), P("tower", None, None), P(), P(), P())
    return jax.shard_map(
        on_device, mesh=mesh, in_specs=placed, out_specs=P("tower", "blk", None), check_vma=False
    )
```

```python
import functools

import jax
import jax.numpy as jnp
from jax import lax
from jax.experimental import pallas as pl
from jax.experimental.pallas import tpu as pltpu
from jax.sharding import PartitionSpec as P

MESH = pl.DeviceIdType.MESH
FIRST, LATER, NEAR, LAG = 11, 15, 1.5, 4


def grid_of(blocks):
    chips = blocks // 2
    across = 1
    while (2 * across) ** 2 <= chips and chips % (2 * across) == 0:
        across *= 2
    return chips // across, across


def by_distance(size):
    return [sorted(range(size), key=lambda other: (abs(other - here), other)) for here in range(size)]


def pick(table, here, step):
    value = jnp.int32(table[0][step])
    for place in range(1, len(table)):
        value = jnp.where(here == place, jnp.int32(table[place][step]), value)
    return value


def kernel(
    sizes, log_scale, bias, pooled_hbm, gain_hbm, ids_hbm, weight, out,
    held, local, near, pooled, gain, ids, weights, head, coef, fetch_sem, weight_sem,
    got, near_got, sent_x, sent_near, sent_over, sent_level,
    sent_up, sent_down, sent_right, sent_left, sent_core,
):
    depth, across, pieces = sizes
    swap = across == 2
    level = swap and pieces > 1 and depth % 2 == 0
    rows, width = pooled.shape
    part = rows // pieces
    tower = lax.axis_index("tower")
    mine = lax.axis_index("blk")
    core = lax.rem(mine, 2)
    chip = lax.div(mine, 2)
    y = lax.rem(chip, across)
    z = lax.div(chip, across)

    fetches = [
        pltpu.make_async_copy(pooled_hbm, pooled, fetch_sem.at[0]),
        pltpu.make_async_copy(gain_hbm, gain, fetch_sem.at[1]),
        pltpu.make_async_copy(ids_hbm, ids, fetch_sem.at[2]),
    ]
    for fetch in fetches:
        fetch.start()
    slices = weight_sem.shape[0]
    columns = [pl.ds(s * (width // slices), width // slices) for s in range(slices)]
    weight_fetches = [
        pltpu.make_async_copy(weight.at[:, columns[s]], weights.at[:, columns[s]], weight_sem.at[s])
        for s in range(slices)
    ]
    for fetch in weight_fetches:
        fetch.start()

    def at(z_to, y_to, core_to):
        return (z_to * across + y_to) * 2 + core_to

    up, down = at(z + 1, y, core), at(z - 1, y, core)
    right, left = at(z, y + 1, core), at(z, y - 1, core)
    twin = at(z, y, 1 - core)
    has_up, has_down = z < depth - 1, z > 0
    has_right, has_left = y < across - 1, y > 0

    barrier = pltpu.get_barrier_semaphore()

    def greet(tower_to, blk_to):
        pl.semaphore_signal(barrier, inc=1, device_id={"tower": tower_to, "blk": blk_to}, device_id_type=MESH)

    greet(1 - tower, mine)
    greet(tower, twin)
    for there, who in ((has_up, up), (has_down, down), (has_right, right), (has_left, left)):
        pl.when(there)(functools.partial(greet, tower, who))

    fetches[0].wait()
    fetches[1].wait()
    values = pooled[...].astype(jnp.float32)
    center = values - jnp.mean(values, axis=-1, keepdims=True)
    spread = jnp.mean(center * center, axis=-1, keepdims=True)
    normed = (center * lax.rsqrt(spread + 1e-06) * gain[...]).astype(jnp.bfloat16)
    length = jnp.zeros((rows, 1), jnp.float32)
    for s in range(slices):
        weight_fetches[s].wait()
        piece = jnp.dot(normed, weights[:, columns[s]], preferred_element_type=jnp.float32)
        length += jnp.sum(piece * piece, axis=-1, keepdims=True)
        head[:, columns[s]] = piece
    local[...] = (head[...] * lax.rsqrt(length + 1e-06)).astype(jnp.bfloat16)

    count = (
        2
        + has_up.astype(jnp.int32)
        + has_down.astype(jnp.int32)
        + has_right.astype(jnp.int32)
        + has_left.astype(jnp.int32)
    )
    pl.semaphore_wait(barrier, count)

    def span(k):
        return pl.ds(k * part, part)

    def cross(k):
        return pltpu.make_async_remote_copy(
            src_ref=local.at[span(k)],
            dst_ref=held.at[mine, span(k)],
            send_sem=sent_x.at[k],
            recv_sem=got.at[mine, k],
            device_id={"tower": 1 - tower, "blk": mine},
            device_id_type=MESH,
        )

    def relay(block, k, sem, who):
        return pltpu.make_async_remote_copy(
            src_ref=held.at[block, span(k)],
            dst_ref=held.at[block, span(k)],
            send_sem=sem,
            recv_sem=got.at[block, k],
            device_id={"tower": tower, "blk": who},
            device_id_type=MESH,
        )

    beside = at(z, 1 - y, core)

    def step_near(k):
        return pltpu.make_async_remote_copy(
            src_ref=local.at[span(k)],
            dst_ref=near.at[span(k)],
            send_sem=sent_near.at[k],
            recv_sem=near_got.at[k],
            device_id={"tower": tower, "blk": beside},
            device_id_type=MESH,
        )

    def step_over(k):
        return pltpu.make_async_remote_copy(
            src_ref=near.at[span(k)],
            dst_ref=held.at[beside, span(k)],
            send_sem=sent_over.at[k],
            recv_sem=got.at[beside, k],
            device_id={"tower": 1 - tower, "blk": mine},
            device_id_type=MESH,
        )

    pair_z = z + 1 - 2 * lax.rem(z, 2)

    def step_level():
        return relay(beside, pieces - 1, sent_level.at[0], at(pair_z, y, core))

    for k in range(pieces):
        cross(k).start()
        if swap:
            step_near(k).start()

    z_table, y_table = by_distance(depth), by_distance(across)
    z_at = [pick(z_table, z, j) for j in range(depth)]
    y_at = [pick(y_table, y, i) for i in range(across)]

    def lines(here, size, there):
        found = [(0, here, None)]
        for step in range(1, size):
            found.append((step, here - step, here >= step))
            found.append((step, here + step, here + step < size))
        return found

    sources = [
        (dz, dy, z_from, y_from, [test for test in (z_test, y_test) if test is not None])
        for dz, z_from, z_test in lines(z, depth, z)
        for dy, y_from, y_test in lines(y, across, y)
    ]

    def guarded(tests, action):
        if tests:
            pl.when(functools.reduce(jnp.logical_and, tests))(action)
        else:
            action()

    def sends(source, k):
        dz, dy, z_from, y_from, tests = source
        block = at(z_from, y_from, core)
        found = []
        if dy == 0:
            found.append(([has_up, z_from <= z], relay(block, k, sent_up.at[z_from, k], up)))
            found.append(([has_down, z_from >= z], relay(block, k, sent_down.at[z_from, k], down)))
        if not (swap and (dz == 0 or dy > 0)):
            over = []
            if level and dz == 1 and k == pieces - 1:
                over = [z_from != pair_z]
            found.append(
                ([has_right, y_from <= y] + over, relay(block, k, sent_right.at[z_from, y_from, k], right))
            )
            found.append(
                ([has_left, y_from >= y] + over, relay(block, k, sent_left.at[z_from, y_from, k], left))
            )
        if level and dz == 0 and dy == 1 and k == pieces - 1:
            found.append(([], step_level()))
        found.append(([], relay(block, k, sent_core.at[z_from, y_from, k], twin)))
        return [(tests + more, copy) for more, copy in found]

    def arrive(source, k):
        dz, dy, z_from, y_from, tests = source

        def land():
            block = at(z_from, y_from, core)
            relay(block, k, sent_core.at[z_from, y_from, k], twin).wait_recv()
            for more, copy in sends(source, k):
                guarded(more[len(tests) :], copy.start)

        guarded(tests, land)

    def due(dz, dy, k):
        if dy == 0:
            return 1 + k if dz == 0 else 3 + 4 * (dz - 1) + k
        if dz == 0:
            return (FIRST if swap else 4) + 4 * (dy - 1) + k
        return LATER + 4 * (dz - 1) + 4 * (dy - 1) + k

    fetches[2].wait()
    scale = jnp.exp(jnp.full((1, rows), log_scale[0], jnp.float32))
    shift = bias[0]
    own_ids = jnp.transpose(jnp.broadcast_to(ids[pl.ds(mine, 1), :], (rows, rows)))
    out[...] = jnp.zeros_like(out)

    def forces(j, i):
        group = z_at[j] * across + y_at[i]
        other = 2 * group + 1 - core
        for k in range(pieces):
            relay(other, k, sent_core.at[0, 0, k], twin).wait_recv()
        moving = held[pl.ds(2 * group, 2)].reshape(2 * rows, -1)
        dots = lax.dot_general(
            local[...], moving, (((1,), (1,)), ((), ())), preferred_element_type=jnp.float32
        )
        for half in range(2):
            logits = scale * dots[:, half * rows : (half + 1) * rows] + shift
            same = own_ids == ids[pl.ds(2 * group + half, 1), :]
            sign = jnp.where(same, jnp.float32(1.0), jnp.float32(-1.0))
            coef[:, half * rows : (half + 1) * rows] = (
                -sign / (1.0 + jnp.exp(sign * logits))
            ).astype(jnp.bfloat16)
        out[...] += jnp.dot(coef[...], moving, preferred_element_type=jnp.float32)

    events = []
    for k in range(pieces):
        for source in sources:
            events.append((due(source[0], source[1], k), functools.partial(arrive, source, k)))
        if swap:

            def pass_over(k=k):
                step_near(k).wait_recv()
                step_over(k).start()

            events.append((k + NEAR, pass_over))
    for j in range(depth):
        for i in range(across):
            events.append((due(j, i, pieces - 1) + LAG, functools.partial(forces, j, i)))
    events.sort(key=lambda event: event[0])
    for _, action in events:
        action()

    for k in range(pieces):
        cross(k).wait_send()
        if swap:
            step_near(k).wait_send()
            step_over(k).wait_send()
    for source in sources:
        for k in range(pieces):
            for tests, copy in sends(source, k):
                guarded(tests, copy.wait_send)


def solution(mesh):
    blocks = mesh.shape["blk"]
    depth, across = grid_of(blocks)
    pieces = 4 if blocks <= 16 else 1

    def on_device(pooled, final_gain, head_weight, pair_ids, log_scale, bias):
        _, rows, width = pooled.shape
        smem = pl.BlockSpec(memory_space=pltpu.SMEM)
        hbm = pl.BlockSpec(memory_space=pltpu.HBM)
        dma = pltpu.SemaphoreType.DMA
        slices = 3 if width % 384 == 0 else 1
        grant = 67043328 - 4 * rows * width - 2**17
        total = pl.pallas_call(
            functools.partial(kernel, (depth, across, pieces)),
            name="tower_forces",
            out_shape=pltpu.VMEM((rows, width), jnp.float32),
            in_specs=[smem, smem, hbm, hbm, hbm, hbm],
            out_specs=pl.BlockSpec(memory_space=pltpu.VMEM),
            scratch_shapes=[
                pltpu.VMEM((blocks, rows, width), jnp.bfloat16),
                pltpu.VMEM((rows, width), jnp.bfloat16),
                pltpu.VMEM((rows, width), jnp.bfloat16),
                pltpu.VMEM((rows, width), jnp.bfloat16),
                pltpu.VMEM((1, width), jnp.float32),
                pltpu.VMEM((blocks, rows), jnp.int32),
                pltpu.VMEM((width, width), jnp.bfloat16),
                pltpu.VMEM((rows, width), jnp.float32),
                pltpu.VMEM((rows, 2 * rows), jnp.bfloat16),
                dma((3,)),
                dma((slices,)),
                dma((blocks, pieces)),
                dma((pieces,)),
                dma((pieces,)),
                dma((pieces,)),
                dma((pieces,)),
                dma((1,)),
                dma((depth, pieces)),
                dma((depth, pieces)),
                dma((depth, across, pieces)),
                dma((depth, across, pieces)),
                dma((depth, across, pieces)),
            ],
            compiler_params=pltpu.CompilerParams(
                collective_id=0, has_side_effects=True, vmem_limit_bytes=grant
            ),
        )(log_scale, bias, pooled[0], final_gain, pair_ids.reshape(blocks, rows), head_weight[0])
        return total[None]

    placed = (P("tower", "blk", None), P("tower", None), P("tower", None, None), P(), P(), P())
    return jax.shard_map(
        on_device, mesh=mesh, in_specs=placed, out_specs=P("tower", "blk", None), check_vma=False
    )
```
